256 devices in a mesh: lvl: 16 (over y_hi, z), lon: 16 (over x, y_lo, core).
Axes of the slice: x: 4, y: 4 (y_hi: 2, y_lo: 2; y = y_hi * 2 + y_lo), z: 8, core: 2. Of those that a mesh axis runs over, the one named last changes fastest.
Arguments:
- window: float32 [16, 16, 69, 2048], P('lvl', None, None, 'lon'), may hold values from -6 to 6
- anchor: float32 [16, 69, 2048], P(None, None, 'lon'), may hold values from -6 to 6
- noise: float32 [16, 16, 69, 2048], P('lvl', None, None, 'lon'), may hold values from -6 to 6
- conv_in: bfloat16 [3, 3, 192, 69], replicated, may hold values from -0.25 to 0.25
- conv_out: bfloat16 [3, 3, 69, 192], replicated, may hold values from -0.15625 to 0.15625
- time_shift: float32 [192], replicated, may hold values from -4 to 4
- plan: int32 [256], replicated, may hold values from 0 to 999, as said below
- start: int32 [1], replicated, may hold values from 0 to 239
Outputs:
- advanced: float32 [16, 16, 69, 2048], P('lvl', None, None, 'lon')
The draws below stay inside these ranges and needn't reach their ends.
Inputs may be any that keep to these rules, and one draw needn't show every extreme that they name: `plan`: strictly decreasing, first entry 999.
All inputs are finite; a program needn't handle non-finite values.
Results may differ from the reference program's by a relative error of at most 0.0003.
Values may be sent and summed in bfloat16 or wider, within the bound.
A program may use at most 64 MiB of HBM per device.

```python
import jax
import jax.numpy as jnp

CIN = 69
HID = 192
LAT = 16
SWEEPS = 2
TABLE = 256
LEVELS = 16
LON = 2048


def draw_plan(key, part):
    gaps = jax.random.randint(key, (TABLE,), 1, 4)
    return (999 - (jnp.cumsum(gaps) - gaps[0])).astype(jnp.int32)


def level_of(key, extent, split, least, high):
    def one(dim, shards_of):
        heights = jax.random.uniform(jax.random.fold_in(jax.random.fold_in(key, 6), dim), (shards_of,), jnp.float32, least / len(split), high / len(split))
        return jnp.repeat(jnp.exp(heights), extent[dim] // shards_of).reshape((-1,) + (1,) * (len(extent) - dim - 1))

    level = one(*split[0])
    for cut in split[1:]:
        level = level * one(*cut)
    return level


def normal_values(key, extent, deviation, bound, split=(), dtype=jnp.bfloat16):
    result = jax.random.normal(key, extent, jnp.float32) * deviation
    if len(split) > 0:
        result = level_of(key, extent, split, -0.22, 0.18) * result
    return jnp.clip(result, min=-bound, max=bound).astype(dtype)


def setup_inputs(seed: int = 0) -> dict:
    seeds = jax.random.split(jax.random.key(seed), 9)
    return {
        "window": normal_values(seeds[0], (LEVELS, LAT, CIN, LON), 1.0, 6.0, ((0, 16), (3, 16)), jnp.float32),
        "anchor": normal_values(seeds[1], (LAT, CIN, LON), 1.0, 6.0, ((2, 16),), jnp.float32),
        "noise": normal_values(seeds[2], (LEVELS, LAT, CIN, LON), 1.0, 6.0, ((0, 16), (3, 16)), jnp.float32),
        "conv_in": normal_values(seeds[3], (3, 3, HID, CIN), (9 * CIN) ** -0.5, 0.25),
        "conv_out": normal_values(seeds[4], (3, 3, CIN, HID), (9 * HID) ** -0.5, 0.15625),
        "time_shift": normal_values(seeds[5], (HID,), 1.0, 4.0, (), jnp.float32),
        "plan": draw_plan(jax.random.fold_in(seeds[8], 71), 0),
        "start": jax.random.randint(seeds[7], (1,), 0, TABLE - LEVELS).astype(jnp.int32),
    }


def convolve(field, weight):
    wrapped = jnp.concatenate([field[:, :, -1:], field, field[:, :, :1]], axis=2)
    padded = jnp.pad(wrapped, ((1, 1), (0, 0), (0, 0)))
    rows = field.shape[0]
    cols = field.shape[2]
    total = jnp.zeros((rows, weight.shape[2], cols), jnp.float32)
    for a in range(3):
        for b in range(3):
            piece = padded[a:a + rows, :, b:b + cols].astype(jnp.float32)
            total = total + jnp.einsum('oc,lcn->lon', weight[a, b].astype(jnp.float32), piece)
    return total

def reference(window, anchor, noise, conv_in, conv_out, time_shift, plan, start):
    first = start[0]
    times = jax.lax.dynamic_slice(plan, (first,), (LEVELS + 1,)).astype(jnp.float32)
    t_now = times[:-1]
    t_next = times[1:]
    beta = 0.1 + 19.9 * t_now / 1000.0
    step = (t_now - t_next) / 1000.0
    states = window
    inclusive = None
    for sweep in range(SWEEPS):
        incs = []
        for level in range(LEVELS):
            state = states[level]
            xb = state.astype(jnp.bfloat16)
            pre = convolve(xb, conv_in)
            hidden = jax.nn.silu(pre + t_now[level] / 1000.0 * time_shift[None, :, None]).astype(jnp.bfloat16)
            score = convolve(hidden, conv_out)
            inc = (0.5 * beta[level] * state + beta[level] * score) * step[level] + jnp.sqrt(beta[level] * step[level]) * noise[level]
            incs.append(inc)
        incs = jnp.stack(incs)
        inclusive = jnp.cumsum(incs, axis=0)
        states = anchor[None] + (inclusive - incs)
    return anchor[None] + inclusive
```

```python
import functools

import jax
import jax.numpy as jnp
from jax import lax
from jax.experimental import pallas as pl
from jax.experimental.pallas import tpu as pltpu
from jax.sharding import PartitionSpec as P

MESH = pl.DeviceIdType.MESH
F32 = jnp.float32
BF16 = jnp.bfloat16

RING = 8
HOP = 3
CROSS = 4
HALO = 3


def kernel(
    window, anchor, noise, conv_in, conv_out, time_shift, plan, start, out,
    xb, halo, xs, hid, w1, w2, coef, shift, state, inc,
    pin, pout, sin, sout, tin, tout,
    hsend, hrecv, psend, precv, ssend, srecv, tsend, trecv,
):
    lats, cin, width = window.shape
    hidden = time_shift.shape[1]
    step_c = 80
    last = RING - 1
    lvl = lax.axis_index("lvl")
    lon = lax.axis_index("lon")
    nlon = lax.axis_size("lon")
    ring = lvl // RING
    z = lvl % RING
    right = lax.rem(lon + 1, nlon)
    left = lax.rem(lon + nlon - 1, nlon)
    base = ring * RING
    above = base + lax.rem(z + 1, RING)
    below = base + lax.rem(z + RING - 1, RING)
    other = (1 - ring) * RING + z

    barrier = pltpu.get_barrier_semaphore()
    for target in ((lvl, left), (lvl, right), (above, lon), (below, lon), (other, lon)):
        pl.semaphore_signal(barrier, inc=1, device_id=target, device_id_type=MESH)

    t_now = plan[start[0] + lvl]
    t_next = plan[start[0] + lvl + 1]
    tv = jnp.full((8, width), t_now.astype(F32))
    uv = jnp.full((8, width), t_next.astype(F32))
    beta = 0.1 + 19.9 * tv / 1000.0
    dt = (tv - uv) / 1000.0
    coef[0] = beta
    coef[1] = dt
    coef[2] = jnp.sqrt(beta * dt)
    rows = lax.broadcasted_iota(jnp.int32, (hidden, hidden), 0)
    cols = lax.broadcasted_iota(jnp.int32, (hidden, hidden), 1)
    spread = jnp.where(rows == cols, jnp.broadcast_to(time_shift[...], (hidden, hidden)), 0.0)
    column = jnp.sum(spread, axis=1, keepdims=True)
    shift[...] = jnp.broadcast_to(column, (hidden, width)) * (tv[0:1, :] / 1000.0)
    w1[...] = jnp.zeros_like(w1)
    w2[...] = jnp.zeros_like(w2)
    for a in range(3):
        for b in range(3):
            w1[a, :, b * step_c : b * step_c + cin] = conv_in[a, b]
            w2[a, b * step_c : b * step_c + cin, :] = conv_out[a, b]
    xs[...] = jnp.zeros_like(xs)
    hid[...] = jnp.zeros_like(hid)

    @pl.when(z == 0)
    def _():
        pin[...] = jnp.zeros_like(pin)

    @pl.when(z == last)
    def _():
        sin[...] = jnp.zeros_like(sin)

    @pl.when(ring == 0)
    def _():
        tin[...] = jnp.zeros_like(tin)

    pl.semaphore_wait(barrier, 5)

    def halo_copy(s, side, l):
        target = right if side == 0 else left
        return pltpu.make_async_remote_copy(
            src_ref=xb.at[s, l], dst_ref=halo.at[s, side, l],
            send_sem=hsend.at[s, side, l], recv_sem=hrecv.at[s, side, l],
            device_id=(lvl, target), device_id_type=MESH,
        )

    def chain_copy(src, dst, send, recv, target, s, l):
        return pltpu.make_async_remote_copy(
            src_ref=src.at[s, l], dst_ref=dst.at[s, l],
            send_sem=send.at[s, l], recv_sem=recv.at[s, l],
            device_id=(target, lon), device_id_type=MESH,
        )

    def p_copy(s, l):
        return chain_copy(pout, pin, psend, precv, above, s, l)

    def s_copy(s, l):
        return chain_copy(sout, sin, ssend, srecv, below, s, l)

    def t_copy(s, l):
        return chain_copy(tout, tin, tsend, trecv, other, s, l)

    def first(l, carry):
        xb[0, l] = window[l].astype(BF16)
        halo_copy(0, 0, l).start()
        halo_copy(0, 1, l).start()
        return carry

    lax.fori_loop(0, lats, first, 0)

    lane = lax.broadcasted_iota(jnp.int32, (cin, width), 1)

    def place(s, l):
        halo_copy(s, 0, l).wait_recv()
        halo_copy(s, 1, l).wait_recv()
        main = xb[s, l].astype(F32)
        from_left = halo[s, 0, l].astype(F32)
        from_right = halo[s, 1, l].astype(F32)
        edge = jnp.where(lane < width // 2, from_right, from_left)
        up = pltpu.roll(main, 1, axis=1)
        down = pltpu.roll(main, width - 1, axis=1)
        edge_up = pltpu.roll(edge, 1, axis=1)
        edge_down = pltpu.roll(edge, width - 1, axis=1)
        low = lane == 0
        high = lane == width - 1
        xs[s, l + 1, 0:cin, 0:width] = jnp.where(low, edge_up, up).astype(BF16)
        xs[s, l + 1, 0:cin, width:] = jnp.where(low, up, edge_up).astype(BF16)
        xs[s, l + 1, step_c : step_c + cin, 0:width] = main.astype(BF16)
        xs[s, l + 1, step_c : step_c + cin, width:] = edge.astype(BF16)
        xs[s, l + 1, 2 * step_c : 2 * step_c + cin, 0:width] = jnp.where(high, edge_down, down).astype(BF16)
        xs[s, l + 1, 2 * step_c : 2 * step_c + cin, width:] = jnp.where(high, down, edge_down).astype(BF16)

    def activate(s, l):
        total = jnp.dot(w1[0], xs[s, l], preferred_element_type=F32)
        total += jnp.dot(w1[1], xs[s, l + 1], preferred_element_type=F32)
        total += jnp.dot(w1[2], xs[s, l + 2], preferred_element_type=F32)
        offset = shift[...]
        v = total + jnp.concatenate([offset, offset], axis=1)
        hid[s, l + 1] = (v / (1.0 + jnp.exp(-v))).astype(BF16)

    lane8 = lax.broadcasted_iota(jnp.int32, (step_c, width), 1)

    def advance(s, l, current):
        total = jnp.dot(w2[0], hid[s, l], preferred_element_type=F32)
        total += jnp.dot(w2[1], hid[s, l + 1], preferred_element_type=F32)
        total += jnp.dot(w2[2], hid[s, l + 2], preferred_element_type=F32)
        before = total[0:step_c]
        middle = total[step_c : 2 * step_c]
        after = total[2 * step_c : 3 * step_c]
        a0 = pltpu.roll(before[:, 0:width], 1, axis=1)
        a1 = pltpu.roll(before[:, width:], 1, axis=1)
        c0 = pltpu.roll(after[:, 0:width], width - 1, axis=1)
        c1 = pltpu.roll(after[:, width:], width - 1, axis=1)
        score = jnp.where(lane8 == 0, a1, a0) + middle[:, 0:width] + jnp.where(lane8 == width - 1, c1, c0)
        score = score[0:cin]
        bv, dv, nv = coef[0, 0:1], coef[1, 0:1], coef[2, 0:1]
        inc[s, l] = (0.5 * bv * current + bv * score) * dv + nv * noise[l]

    def inside(l):
        return jnp.logical_and(l >= 0, l < lats)

    def chain_p(s, l):
        @pl.when(z > 0)
        def _():
            p_copy(s, l).wait_recv()

        @pl.when(z < last)
        def _():
            pout[s, l] = pin[s, l] + inc[s, l]
            p_copy(s, l).start()

    def chain_s(s, l):
        @pl.when(z < last)
        def _():
            s_copy(s, l).wait_recv()

        sout[s, l] = sin[s, l] + inc[s, l]

        @pl.when(z > 0)
        def _():
            s_copy(s, l).start()

    far = jnp.maximum(z, last - z)
    ready = jnp.where(ring == 0, HOP * z, HOP * far + CROSS)
    second_p = jnp.where(ring == 0, HOP * z, HOP * last + CROSS + HOP * z)
    second_s = HOP * last + HOP * (last - z)
    finish = jnp.where(ring == 0, HOP * z, HOP * last + CROSS + HOP * far)
    begin2 = 4 + HALO
    steps = lats + begin2 + HOP * last + CROSS + HOP * last

    def step(t, carry):
        @pl.when(t < lats)
        def _():
            place(0, t)

        @pl.when(inside(t - 1))
        def _():
            activate(0, t - 1)

        @pl.when(inside(t - 2))
        def _():
            advance(0, t - 2, window[t - 2])

        lp = t - 2 - HOP * z

        @pl.when(inside(lp))
        def _():
            chain_p(0, lp)

        @pl.when(ring == 0)
        def _():
            ls = t - 2 - HOP * (last - z)

            @pl.when(inside(ls))
            def _():
                chain_s(0, ls)

            lt = t - 2 - HOP * far

            @pl.when(inside(lt))
            def _():
                tout[0, lt] = pin[0, lt] + sout[0, lt]
                t_copy(0, lt).start()

        le = t - 2 - ready

        @pl.when(inside(le))
        def _():
            @pl.when(ring == 1)
            def _():
                t_copy(0, le).wait_recv()

            x = anchor[le] + (pin[0, le] + tin[0, le])
            state[le] = x
            xb[1, le] = x.astype(BF16)
            halo_copy(1, 0, le).start()
            halo_copy(1, 1, le).start()

        lx = le - HALO

        @pl.when(inside(lx))
        def _():
            place(1, lx)

        @pl.when(inside(lx - 1))
        def _():
            activate(1, lx - 1)

        @pl.when(inside(lx - 2))
        def _():
            advance(1, lx - 2, state[lx - 2])

        lq = t - begin2 - second_p

        @pl.when(inside(lq))
        def _():
            chain_p(1, lq)

        @pl.when(ring == 0)
        def _():
            lr = t - begin2 - second_s

            @pl.when(inside(lr))
            def _():
                chain_s(1, lr)
                tout[1, lr] = pin[1, lr] + sout[1, lr]
                t_copy(1, lr).start()

        lf = t - begin2 - finish

        @pl.when(inside(lf))
        def _():
            @pl.when(ring == 1)
            def _():
                t_copy(1, lf).wait_recv()

            out[lf] = anchor[lf] + (pin[1, lf] + tin[1, lf] + inc[1, lf])

        return carry

    lax.fori_loop(0, steps, step, 0)

    def drain(l, carry):
        for s in range(2):
            halo_copy(s, 0, l).wait_send()
            halo_copy(s, 1, l).wait_send()

            @pl.when(z < last)
            def _():
                p_copy(s, l).wait_send()

            @pl.when(ring == 0)
            def _():
                t_copy(s, l).wait_send()

                @pl.when(z > 0)
                def _():
                    s_copy(s, l).wait_send()

        return carry

    lax.fori_loop(0, lats, drain, 0)


def body(window, anchor, noise, conv_in, conv_out, time_shift, plan, start):
    _, lats, cin, width = window.shape
    hidden = time_shift.shape[0]
    vmem = pl.BlockSpec(memory_space=pltpu.VMEM)
    smem = pl.BlockSpec(memory_space=pltpu.SMEM)
    rows = (2, lats, cin, width)
    dma = pltpu.SemaphoreType.DMA
    out = pl.pallas_call(
        kernel,
        out_shape=jax.ShapeDtypeStruct((lats, cin, width), F32),
        in_specs=[vmem] * 6 + [smem] * 2,
        out_specs=vmem,
        scratch_shapes=[
            pltpu.VMEM(rows, BF16),
            pltpu.VMEM((2,) + rows, BF16),
            pltpu.VMEM((2, lats + 2, 256, 2 * width), BF16),
            pltpu.VMEM((2, lats + 2, hidden, 2 * width), BF16),
            pltpu.VMEM((3, hidden, 256), BF16),
            pltpu.VMEM((3, 240, hidden), BF16),
            pltpu.VMEM((3, 8, width), F32),
            pltpu.VMEM((hidden, width), F32),
            pltpu.VMEM((lats, cin, width), F32),
            pltpu.VMEM(rows, F32),
        ]
        + [pltpu.VMEM(rows, F32)] * 6
        + [dma((2, 2, lats))] * 2
        + [dma((2, lats))] * 6,
        compiler_params=pltpu.CompilerParams(
            collective_id=0, has_side_effects=True, vmem_limit_bytes=56 * 1024 * 1024
        ),
    )(window[0], anchor, noise[0], conv_in, conv_out, time_shift[None, :], plan, start)
    return out[None]


def solution(mesh):
    return jax.shard_map(
        body,
        mesh=mesh,
        in_specs=(
            P("lvl", None, None, "lon"),
            P(None, None, "lon"),
            P("lvl", None, None, "lon"),
            P(),
            P(),
            P(),
            P(),
            P(),
        ),
        out_specs=P("lvl", None, None, "lon"),
        check_vma=False,
    )
```

```python
import functools

import jax
import jax.numpy as jnp
from jax import lax
from jax.experimental import pallas as pl
from jax.experimental.pallas import tpu as pltpu
from jax.sharding import PartitionSpec as P

MESH = pl.DeviceIdType.MESH
F32 = jnp.float32
BF16 = jnp.bfloat16

RING = 8
HOP = 3
CROSS = 4
HALO = 3


def kernel(
    window, anchor, noise, conv_in, conv_out, time_shift, plan, start, out,
    xb, halo, xs, hid, w1, w2, wt, coef, shift, state, inc,
    pin, pout, sin, sout, tin, tout,
    hsend, hrecv, psend, precv, ssend, srecv, tsend, trecv, usend,
):
    lats, cin, width = state.shape
    hidden = time_shift.shape[1]
    step_c = 80
    last = RING - 1
    half = RING // 2
    lvl = lax.axis_index("lvl")
    lon = lax.axis_index("lon")
    nlon = lax.axis_size("lon")
    ring = lvl // RING
    z = lvl % RING
    right = lax.rem(lon + 1, nlon)
    left = lax.rem(lon + nlon - 1, nlon)
    base = ring * RING
    above = base + lax.rem(z + 1, RING)
    below = base + lax.rem(z + RING - 1, RING)
    other = (1 - ring) * RING + z

    barrier = pltpu.get_barrier_semaphore()
    for target in ((lvl, left), (lvl, right), (above, lon), (below, lon), (other, lon)):
        pl.semaphore_signal(barrier, inc=1, device_id=target, device_id_type=MESH)

    def row(l):
        return pl.ds(l, cin, stride=lats)

    def convert(l, carry):
        xb[0, l] = window[row(l), :].astype(BF16)
        return carry

    lax.fori_loop(0, lats, convert, 0)

    pl.semaphore_wait(barrier, 5)

    def halo_copy(s, side, l):
        target = right if side == 0 else left
        return pltpu.make_async_remote_copy(
            src_ref=xb.at[s, l], dst_ref=halo.at[s, side, l],
            send_sem=hsend.at[s, side, l], recv_sem=hrecv.at[s, side, l],
            device_id=(lvl, target), device_id_type=MESH,
        )

    def chain_copy(src, dst, send, recv, target, s, l):
        return pltpu.make_async_remote_copy(
            src_ref=src.at[s, l], dst_ref=dst.at[s, l],
            send_sem=send.at[s, l], recv_sem=recv.at[s, l],
            device_id=(target, lon), device_id_type=MESH,
        )

    def p_copy(s, l):
        return chain_copy(pout, pin, psend, precv, above, s, l)

    def s_copy(s, l):
        return chain_copy(sout, sin, ssend, srecv, below, s, l)

    def t_copy(s, l):
        return chain_copy(tout if s == 0 else sout, tin, tsend, trecv, other, s, l)

    def u_copy(l):
        return pltpu.make_async_remote_copy(
            src_ref=sout.at[1, l], dst_ref=sin.at[1, l],
            send_sem=usend.at[l], recv_sem=srecv.at[1, l],
            device_id=(above, lon), device_id_type=MESH,
        )

    def spread_copy(l):
        return chain_copy(sin, tin, tsend, trecv, other, 1, l)

    def relay_copy(l):
        onward = jnp.where(jnp.logical_and(ring == 0, z < half - 1), above, below)
        return chain_copy(sin, sin, ssend, srecv, onward, 1, l)

    def first(l, carry):
        halo_copy(0, 0, l).start()
        halo_copy(0, 1, l).start()
        return carry

    lax.fori_loop(0, lats, first, 0)

    t_now = plan[start[0] + lvl]
    t_next = plan[start[0] + lvl + 1]
    tv = jnp.full((8, width), t_now.astype(F32))
    uv = jnp.full((8, width), t_next.astype(F32))
    beta = 0.1 + 19.9 * tv / 1000.0
    dt = (tv - uv) / 1000.0
    coef[0] = beta
    coef[1] = dt
    coef[2] = jnp.sqrt(beta * dt)
    rows = lax.broadcasted_iota(jnp.int32, (hidden, hidden), 0)
    cols = lax.broadcasted_iota(jnp.int32, (hidden, hidden), 1)
    spread = jnp.where(rows == cols, jnp.broadcast_to(time_shift[...], (hidden, hidden)), 0.0)
    column = jnp.sum(spread, axis=1, keepdims=True)
    shift[...] = jnp.broadcast_to(column, (hidden, width)) * (tv[0:1, :] / 1000.0)
    wt[...] = jnp.zeros_like(wt)
    w2[...] = jnp.zeros_like(w2)
    for a in range(3):
        for b in range(3):
            wt[a, b * step_c : b * step_c + cin, :] = conv_in[a, b]
            w2[a, b * step_c : b * step_c + cin, :] = conv_out[a, b]
    for a in range(3):
        w1[a] = wt[a].T

    blank = jnp.zeros((16, 2 * width), BF16)
    for s in range(2):
        for edge in (0, lats + 1):
            xs[s, edge] = jnp.zeros((256, 2 * width), BF16)
            hid[s, edge] = jnp.zeros((hidden, 2 * width), BF16)

    def clear(l, carry):
        for s in range(2):
            for start_row in (64, 144, 224, 240):
                xs[s, l + 1, start_row : start_row + 16] = blank
        return carry

    lax.fori_loop(0, lats, clear, 0)

    @pl.when(z == 0)
    def _():
        pin[...] = jnp.zeros_like(pin)

    @pl.when(jnp.logical_and(ring == 1, z == half))
    def _():
        pin[1] = jnp.zeros_like(pin[1])

    @pl.when(z == jnp.where(ring == 0, last, half - 1))
    def _():
        sin[...] = jnp.zeros_like(sin)

    @pl.when(ring == 0)
    def _():
        tin[...] = jnp.zeros_like(tin)


    lane = lax.broadcasted_iota(jnp.int32, (cin, width), 1)

    def place(s, l):
        halo_copy(s, 0, l).wait_recv()
        halo_copy(s, 1, l).wait_recv()
        main = xb[s, l].astype(F32)
        from_left = halo[s, 0, l].astype(F32)
        from_right = halo[s, 1, l].astype(F32)
        edge = jnp.where(lane < width // 2, from_right, from_left)
        up = pltpu.roll(main, 1, axis=1)
        down = pltpu.roll(main, width - 1, axis=1)
        edge_up = pltpu.roll(edge, 1, axis=1)
        edge_down = pltpu.roll(edge, width - 1, axis=1)
        low = lane == 0
        high = lane == width - 1
        xs[s, l + 1, 0:cin, 0:width] = jnp.where(low, edge_up, up).astype(BF16)
        xs[s, l + 1, 0:cin, width:] = jnp.where(low, up, edge_up).astype(BF16)
        xs[s, l + 1, step_c : step_c + cin, 0:width] = main.astype(BF16)
        xs[s, l + 1, step_c : step_c + cin, width:] = edge.astype(BF16)
        xs[s, l + 1, 2 * step_c : 2 * step_c + cin, 0:width] = jnp.where(high, edge_down, down).astype(BF16)
        xs[s, l + 1, 2 * step_c : 2 * step_c + cin, width:] = jnp.where(high, down, edge_down).astype(BF16)

    def activate(s, l):
        total = jnp.dot(w1[0], xs[s, l], preferred_element_type=F32)
        total += jnp.dot(w1[1], xs[s, l + 1], preferred_element_type=F32)
        total += jnp.dot(w1[2], xs[s, l + 2], preferred_element_type=F32)
        offset = shift[...]
        v = total + jnp.concatenate([offset, offset], axis=1)
        hid[s, l + 1] = (0.5 * v * (1.0 + jnp.tanh(0.5 * v))).astype(BF16)

    lane8 = lax.broadcasted_iota(jnp.int32, (step_c, width), 1)

    def advance(s, l, current):
        total = jnp.dot(w2[0], hid[s, l], preferred_element_type=F32)
        total += jnp.dot(w2[1], hid[s, l + 1], preferred_element_type=F32)
        total += jnp.dot(w2[2], hid[s, l + 2], preferred_element_type=F32)
        before = total[0:step_c]
        middle = total[step_c : 2 * step_c]
        after = total[2 * step_c : 3 * step_c]
        a0 = pltpu.roll(before[:, 0:width], 1, axis=1)
        a1 = pltpu.roll(before[:, width:], 1, axis=1)
        c0 = pltpu.roll(after[:, 0:width], width - 1, axis=1)
        c1 = pltpu.roll(after[:, width:], width - 1, axis=1)
        score = jnp.where(lane8 == 0, a1, a0) + middle[:, 0:width] + jnp.where(lane8 == width - 1, c1, c0)
        score = score[0:cin]
        bv, dv, nv = coef[0, 0:1], coef[1, 0:1], coef[2, 0:1]
        inc[s, l] = (0.5 * bv * current + bv * score) * dv + nv * noise[row(l), :]

    def inside(l):
        return jnp.logical_and(l >= 0, l < lats)

    def chain_p(s, l):
        @pl.when(z > 0)
        def _():
            p_copy(s, l).wait_recv()

        @pl.when(z < last)
        def _():
            pout[s, l] = pin[s, l] + inc[s, l]
            p_copy(s, l).start()

    def chain_s(s, l):
        @pl.when(z < last)
        def _():
            s_copy(s, l).wait_recv()

        sout[s, l] = sin[s, l] + inc[s, l]

        @pl.when(z > 0)
        def _():
            s_copy(s, l).start()

    far = jnp.maximum(z, last - z)
    ready = jnp.where(ring == 0, HOP * z, HOP * far + CROSS)
    low = z < half
    tail = HOP * last + CROSS
    second_p = jnp.where(ring == 0, HOP * z, jnp.where(low, tail + HOP * z, ready))
    away = jnp.where(z < half - 1, z + 1, last - z)
    path = lax.rem(half - 1 - z + RING, RING)
    reach = HOP * (last + away) + CROSS
    trail = HOP * (half + path) + CROSS
    second_s = jnp.where(ring == 0, HOP * (last + away), trail)
    finish = jnp.where(ring == 0, HOP * z, jnp.maximum(reach, jnp.where(low, tail + HOP * z, trail)))
    source = z == jnp.where(ring == 0, last, half - 1)
    first_of_part = jnp.logical_or(z == 0, jnp.logical_and(ring == 1, z == half))
    last_of_part = jnp.logical_or(z == last, jnp.logical_and(ring == 1, z == half - 1))
    begin2 = 4 + HALO
    steps = lats + begin2 + HOP * (last + half) + CROSS

    def step(t, carry):
        @pl.when(t < lats)
        def _():
            place(0, t)

        @pl.when(inside(t - 1))
        def _():
            activate(0, t - 1)

        @pl.when(inside(t - 2))
        def _():
            advance(0, t - 2, window[row(t - 2), :])

        lp = t - 2 - HOP * z

        @pl.when(inside(lp))
        def _():
            chain_p(0, lp)

        @pl.when(ring == 0)
        def _():
            ls = t - 2 - HOP * (last - z)

            @pl.when(inside(ls))
            def _():
                chain_s(0, ls)

            lt = t - 2 - HOP * far

            @pl.when(inside(lt))
            def _():
                tout[0, lt] = pin[0, lt] + sout[0, lt]
                t_copy(0, lt).start()

        le = t - 2 - ready

        @pl.when(inside(le))
        def _():
            @pl.when(ring == 1)
            def _():
                t_copy(0, le).wait_recv()

            x = anchor[row(le), :] + (pin[0, le] + tin[0, le])
            state[le] = x
            xb[1, le] = x.astype(BF16)
            halo_copy(1, 0, le).start()
            halo_copy(1, 1, le).start()

        lx = le - HALO

        @pl.when(inside(lx))
        def _():
            place(1, lx)

        @pl.when(inside(lx - 1))
        def _():
            activate(1, lx - 1)

        @pl.when(inside(lx - 2))
        def _():
            advance(1, lx - 2, state[lx - 2])

        lq = t - begin2 - second_p

        @pl.when(inside(lq))
        def _():
            @pl.when(jnp.logical_not(first_of_part))
            def _():
                p_copy(1, lq).wait_recv()

            @pl.when(jnp.logical_not(last_of_part))
            def _():
                pout[1, lq] = pin[1, lq] + inc[1, lq]
                p_copy(1, lq).start()

        lr = t - begin2 - second_s

        @pl.when(inside(lr))
        def _():
            @pl.when(jnp.logical_not(source))
            def _():
                s_copy(1, lr).wait_recv()

            @pl.when(ring == 0)
            def _():
                @pl.when(z == last)
                def _():
                    sout[1, lr] = pin[1, lr] + inc[1, lr]
                    u_copy(lr).start()
                    s_copy(1, lr).start()
                    t_copy(1, lr).start()

                @pl.when(z < last)
                def _():
                    spread_copy(lr).start()

                @pl.when(jnp.logical_or(z < half - 2, jnp.logical_and(z >= half, z < last)))
                def _():
                    relay_copy(lr).start()

            @pl.when(ring == 1)
            def _():
                @pl.when(z == half - 1)
                def _():
                    sout[1, lr] = inc[1, lr]
                    s_copy(1, lr).start()

                @pl.when(z < half - 1)
                def _():
                    sout[1, lr] = sin[1, lr] + inc[1, lr]
                    s_copy(1, lr).start()

                @pl.when(z > half)
                def _():
                    relay_copy(lr).start()

        lf = t - begin2 - finish

        @pl.when(inside(lf))
        def _():
            @pl.when(ring == 1)
            def _():
                t_copy(1, lf).wait_recv()

            total = pin[1, lf] + tin[1, lf] + inc[1, lf]
            upper = jnp.logical_and(ring == 1, z >= half)

            @pl.when(upper)
            def _():
                out[row(lf), :] = anchor[row(lf), :] + (total + sin[1, lf])

            @pl.when(jnp.logical_not(upper))
            def _():
                out[row(lf), :] = anchor[row(lf), :] + total

        return carry

    lax.fori_loop(0, steps, step, 0)

    ends = jnp.logical_or(z == half - 1, z == half - 2)
    passes = jnp.where(ring == 0, jnp.logical_not(ends), z != half)

    def drain(l, carry):
        for s in range(2):
            halo_copy(s, 0, l).wait_send()
            halo_copy(s, 1, l).wait_send()

            @pl.when(ring == 0)
            def _():
                t_copy(s, l).wait_send()

        @pl.when(z < last)
        def _():
            p_copy(0, l).wait_send()

        @pl.when(jnp.logical_not(last_of_part))
        def _():
            p_copy(1, l).wait_send()

        @pl.when(jnp.logical_and(ring == 0, z > 0))
        def _():
            s_copy(0, l).wait_send()

        @pl.when(passes)
        def _():
            s_copy(1, l).wait_send()

        @pl.when(jnp.logical_and(ring == 0, z == last))
        def _():
            u_copy(l).wait_send()

        return carry

    lax.fori_loop(0, lats, drain, 0)


def rows_of(field):
    lats, cin, width = field.shape
    return field.transpose(1, 0, 2).reshape(cin * lats, width)


def body(window, anchor, noise, conv_in, conv_out, time_shift, plan, start):
    _, lats, cin, width = window.shape
    hidden = time_shift.shape[0]
    vmem = pl.BlockSpec(memory_space=pltpu.VMEM)
    smem = pl.BlockSpec(memory_space=pltpu.SMEM)
    rows = (2, lats, cin, width)
    dma = pltpu.SemaphoreType.DMA
    out = pl.pallas_call(
        kernel,
        out_shape=jax.ShapeDtypeStruct((cin * lats, width), F32),
        in_specs=[vmem] * 6 + [smem] * 2,
        out_specs=vmem,
        scratch_shapes=[
            pltpu.VMEM(rows, BF16),
            pltpu.VMEM((2,) + rows, BF16),
            pltpu.VMEM((2, lats + 2, 256, 2 * width), BF16),
            pltpu.VMEM((2, lats + 2, hidden, 2 * width), BF16),
            pltpu.VMEM((3, hidden, 256), BF16),
            pltpu.VMEM((3, 240, hidden), BF16),
            pltpu.VMEM((3, 256, hidden), BF16),
            pltpu.VMEM((3, 8, width), F32),
            pltpu.VMEM((hidden, width), F32),
            pltpu.VMEM((lats, cin, width), F32),
            pltpu.VMEM(rows, F32),
        ]
        + [pltpu.VMEM(rows, F32)] * 6
        + [dma((2, 2, lats))] * 2
        + [dma((2, lats))] * 6
        + [dma((lats,))],
        compiler_params=pltpu.CompilerParams(
            collective_id=0, has_side_effects=True, vmem_limit_bytes=56 * 1024 * 1024
        ),
    )(
        rows_of(window[0]), rows_of(anchor), rows_of(noise[0]), conv_in.transpose(0, 1, 3, 2),
        conv_out, time_shift[None, :], plan, start,
    )
    return out.reshape(cin, lats, width).transpose(1, 0, 2)[None]


def solution(mesh):
    return jax.shard_map(
        body,
        mesh=mesh,
        in_specs=(
            P("lvl", None, None, "lon"),
            P(None, None, "lon"),
            P("lvl", None, None, "lon"),
            P(),
            P(),
            P(),
            P(),
            P(),
        ),
        out_specs=P("lvl", None, None, "lon"),
        check_vma=False,
    )
```

```python
import functools

import jax
import jax.numpy as jnp
from jax import lax
from jax.experimental import pallas as pl
from jax.experimental.pallas import tpu as pltpu
from jax.sharding import PartitionSpec as P

MESH = pl.DeviceIdType.MESH
F32 = jnp.float32
BF16 = jnp.bfloat16

RING = 8
HOP = 3
CROSS = 4
HALO = 3


def kernel(
    window_hbm, anchor_hbm, noise_hbm, conv_in_hbm, conv_out_hbm, time_shift, plan, start, out,
    window, anchor, noise, conv_in, conv_out, load_sem,
    xb, halo, xs, hid, w1, w2, wt, coef, shift, state, inc,
    pin, pout, sin, sout, tin, tout,
    hsend, hrecv, psend, precv, ssend, srecv, tsend, trecv, usend,
):
    lats, cin, width = state.shape
    hidden = time_shift.shape[1]
    step_c = 80
    last = RING - 1
    half = RING // 2
    lvl = lax.axis_index("lvl")
    lon = lax.axis_index("lon")
    nlon = lax.axis_size("lon")
    ring = lvl // RING
    z = lvl % RING
    right = lax.rem(lon + 1, nlon)
    left = lax.rem(lon + nlon - 1, nlon)
    base = ring * RING
    above = base + lax.rem(z + 1, RING)
    below = base + lax.rem(z + RING - 1, RING)
    other = (1 - ring) * RING + z

    barrier = pltpu.get_barrier_semaphore()
    for target in ((lvl, left), (lvl, right), (above, lon), (below, lon), (other, lon)):
        pl.semaphore_signal(barrier, inc=1, device_id=target, device_id_type=MESH)

    loads = [
        pltpu.make_async_copy(src, dst, load_sem.at[i])
        for i, (src, dst) in enumerate((
            (window_hbm, window), (conv_in_hbm, conv_in), (conv_out_hbm, conv_out),
            (noise_hbm, noise), (anchor_hbm, anchor),
        ))
    ]
    for load in loads:
        load.start()

    def row(l):
        return pl.ds(l, cin, stride=lats)

    def convert(l, carry):
        xb[0, l] = window[row(l), :].astype(BF16)
        return carry

    loads[0].wait()
    lax.fori_loop(0, lats, convert, 0)

    pl.semaphore_wait(barrier, 5)

    def halo_copy(s, side, l):
        target = right if side == 0 else left
        return pltpu.make_async_remote_copy(
            src_ref=xb.at[s, l], dst_ref=halo.at[s, side, l],
            send_sem=hsend.at[s, side, l], recv_sem=hrecv.at[s, side, l],
            device_id=(lvl, target), device_id_type=MESH,
        )

    def chain_copy(src, dst, send, recv, target, s, l):
        return pltpu.make_async_remote_copy(
            src_ref=src.at[s, l], dst_ref=dst.at[s, l],
            send_sem=send.at[s, l], recv_sem=recv.at[s, l],
            device_id=(target, lon), device_id_type=MESH,
        )

    def p_copy(s, l):
        return chain_copy(pout, pin, psend, precv, above, s, l)

    def s_copy(s, l):
        return chain_copy(sout, sin, ssend, srecv, below, s, l)

    def t_copy(s, l):
        return chain_copy(tout if s == 0 else sout, tin, tsend, trecv, other, s, l)

    def u_copy(l):
        return pltpu.make_async_remote_copy(
            src_ref=sout.at[1, l], dst_ref=sin.at[1, l],
            send_sem=usend.at[l], recv_sem=srecv.at[1, l],
            device_id=(above, lon), device_id_type=MESH,
        )

    def spread_copy(l):
        return chain_copy(sin, tin, tsend, trecv, other, 1, l)

    def relay_copy(l):
        onward = jnp.where(jnp.logical_and(ring == 0, z < half - 1), above, below)
        return chain_copy(sin, sin, ssend, srecv, onward, 1, l)

    def first(l, carry):
        halo_copy(0, 0, l).start()
        halo_copy(0, 1, l).start()
        return carry

    lax.fori_loop(0, lats, first, 0)

    t_now = plan[start[0] + lvl]
    t_next = plan[start[0] + lvl + 1]
    tv = jnp.full((8, width), t_now.astype(F32))
    uv = jnp.full((8, width), t_next.astype(F32))
    beta = 0.1 + 19.9 * tv / 1000.0
    dt = (tv - uv) / 1000.0
    coef[0] = beta
    coef[1] = dt
    coef[2] = jnp.sqrt(beta * dt)
    rows = lax.broadcasted_iota(jnp.int32, (hidden, hidden), 0)
    cols = lax.broadcasted_iota(jnp.int32, (hidden, hidden), 1)
    spread = jnp.where(rows == cols, jnp.broadcast_to(time_shift[...], (hidden, hidden)), 0.0)
    column = jnp.sum(spread, axis=1, keepdims=True)
    shift[...] = jnp.broadcast_to(column, (hidden, width)) * (tv[0:1, :] / 1000.0)
    for load in loads[1:]:
        load.wait()
    wt[...] = jnp.zeros_like(wt)
    w2[...] = jnp.zeros_like(w2)
    for a in range(3):
        for b in range(3):
            wt[a, b * step_c : b * step_c + cin, :] = conv_in[a, b]
            w2[a, b * step_c : b * step_c + cin, :] = conv_out[a, b]
    for a in range(3):
        w1[a] = wt[a].T

    blank = jnp.zeros((16, 2 * width), BF16)
    for s in range(2):
        for edge in (0, lats + 1):
            xs[s, edge] = jnp.zeros((256, 2 * width), BF16)
            hid[s, edge] = jnp.zeros((hidden, 2 * width), BF16)

    def clear(l, carry):
        for s in range(2):
            for start_row in (64, 144, 224, 240):
                xs[s, l + 1, start_row : start_row + 16] = blank
        return carry

    lax.fori_loop(0, lats, clear, 0)

    @pl.when(z == 0)
    def _():
        pin[...] = jnp.zeros_like(pin)

    @pl.when(jnp.logical_and(ring == 1, z == half))
    def _():
        pin[1] = jnp.zeros_like(pin[1])

    @pl.when(z == jnp.where(ring == 0, last, half - 1))
    def _():
        sin[...] = jnp.zeros_like(sin)

    @pl.when(ring == 0)
    def _():
        tin[...] = jnp.zeros_like(tin)


    lane = lax.broadcasted_iota(jnp.int32, (cin, width), 1)

    def place(s, l):
        halo_copy(s, 0, l).wait_recv()
        halo_copy(s, 1, l).wait_recv()
        main = xb[s, l].astype(F32)
        from_left = halo[s, 0, l].astype(F32)
        from_right = halo[s, 1, l].astype(F32)
        edge = jnp.where(lane < width // 2, from_right, from_left)
        up = pltpu.roll(main, 1, axis=1)
        down = pltpu.roll(main, width - 1, axis=1)
        edge_up = pltpu.roll(edge, 1, axis=1)
        edge_down = pltpu.roll(edge, width - 1, axis=1)
        low = lane == 0
        high = lane == width - 1
        xs[s, l + 1, 0:cin, 0:width] = jnp.where(low, edge_up, up).astype(BF16)
        xs[s, l + 1, 0:cin, width:] = jnp.where(low, up, edge_up).astype(BF16)
        xs[s, l + 1, step_c : step_c + cin, 0:width] = main.astype(BF16)
        xs[s, l + 1, step_c : step_c + cin, width:] = edge.astype(BF16)
        xs[s, l + 1, 2 * step_c : 2 * step_c + cin, 0:width] = jnp.where(high, edge_down, down).astype(BF16)
        xs[s, l + 1, 2 * step_c : 2 * step_c + cin, width:] = jnp.where(high, down, edge_down).astype(BF16)

    def activate(s, l):
        total = jnp.dot(w1[0], xs[s, l], preferred_element_type=F32)
        total += jnp.dot(w1[1], xs[s, l + 1], preferred_element_type=F32)
        total += jnp.dot(w1[2], xs[s, l + 2], preferred_element_type=F32)
        offset = shift[...]
        v = total + jnp.concatenate([offset, offset], axis=1)
        hid[s, l + 1] = (0.5 * v * (1.0 + jnp.tanh(0.5 * v))).astype(BF16)

    lane8 = lax.broadcasted_iota(jnp.int32, (step_c, width), 1)

    def advance(s, l, current):
        total = jnp.dot(w2[0], hid[s, l], preferred_element_type=F32)
        total += jnp.dot(w2[1], hid[s, l + 1], preferred_element_type=F32)
        total += jnp.dot(w2[2], hid[s, l + 2], preferred_element_type=F32)
        before = total[0:step_c]
        middle = total[step_c : 2 * step_c]
        after = total[2 * step_c : 3 * step_c]
        a0 = pltpu.roll(before[:, 0:width], 1, axis=1)
        a1 = pltpu.roll(before[:, width:], 1, axis=1)
        c0 = pltpu.roll(after[:, 0:width], width - 1, axis=1)
        c1 = pltpu.roll(after[:, width:], width - 1, axis=1)
        score = jnp.where(lane8 == 0, a1, a0) + middle[:, 0:width] + jnp.where(lane8 == width - 1, c1, c0)
        score = score[0:cin]
        bv, dv, nv = coef[0, 0:1], coef[1, 0:1], coef[2, 0:1]
        inc[s, l] = (0.5 * bv * current + bv * score) * dv + nv * noise[row(l), :]

    def inside(l):
        return jnp.logical_and(l >= 0, l < lats)

    def chain_p(s, l):
        @pl.when(z > 0)
        def _():
            p_copy(s, l).wait_recv()

        @pl.when(z < last)
        def _():
            pout[s, l] = pin[s, l] + inc[s, l]
            p_copy(s, l).start()

    def chain_s(s, l):
        @pl.when(z < last)
        def _():
            s_copy(s, l).wait_recv()

        sout[s, l] = sin[s, l] + inc[s, l]

        @pl.when(z > 0)
        def _():
            s_copy(s, l).start()

    far = jnp.maximum(z, last - z)
    ready = jnp.where(ring == 0, HOP * z, HOP * far + CROSS)
    low = z < half
    tail = HOP * last + CROSS
    second_p = jnp.where(ring == 0, HOP * z, jnp.where(low, tail + HOP * z, ready))
    away = jnp.where(z < half - 1, z + 1, last - z)
    path = lax.rem(half - 1 - z + RING, RING)
    reach = HOP * (last + away) + CROSS
    trail = HOP * (half + path) + CROSS
    second_s = jnp.where(ring == 0, HOP * (last + away), trail)
    finish = jnp.where(ring == 0, HOP * z, jnp.maximum(reach, jnp.where(low, tail + HOP * z, trail)))
    source = z == jnp.where(ring == 0, last, half - 1)
    first_of_part = jnp.logical_or(z == 0, jnp.logical_and(ring == 1, z == half))
    last_of_part = jnp.logical_or(z == last, jnp.logical_and(ring == 1, z == half - 1))
    begin2 = 6 + HALO
    steps = lats + begin2 + HOP * (last + half) + CROSS

    def step(t, carry):
        @pl.when(t < lats)
        def _():
            place(0, t)

        @pl.when(jnp.logical_and(t >= 1, t < lats + 3))
        def _():
            done = jnp.clip(t - 3, 0, lats - 1)
            advance(0, done, window[row(done), :])
            activate(0, jnp.minimum(t - 1, lats - 1))

        lp = t - 3 - HOP * z

        @pl.when(inside(lp))
        def _():
            chain_p(0, lp)

        @pl.when(ring == 0)
        def _():
            ls = t - 3 - HOP * (last - z)

            @pl.when(inside(ls))
            def _():
                chain_s(0, ls)

            lt = t - 3 - HOP * far

            @pl.when(inside(lt))
            def _():
                tout[0, lt] = pin[0, lt] + sout[0, lt]
                t_copy(0, lt).start()

        le = t - 3 - ready

        @pl.when(inside(le))
        def _():
            @pl.when(ring == 1)
            def _():
                t_copy(0, le).wait_recv()

            x = anchor[row(le), :] + (pin[0, le] + tin[0, le])
            state[le] = x
            xb[1, le] = x.astype(BF16)
            halo_copy(1, 0, le).start()
            halo_copy(1, 1, le).start()

        lx = le - HALO

        @pl.when(inside(lx))
        def _():
            place(1, lx)

        @pl.when(jnp.logical_and(lx >= 1, lx < lats + 3))
        def _():
            done = jnp.clip(lx - 3, 0, lats - 1)
            advance(1, done, state[done])
            activate(1, jnp.minimum(lx - 1, lats - 1))

        lq = t - begin2 - second_p

        @pl.when(inside(lq))
        def _():
            @pl.when(jnp.logical_not(first_of_part))
            def _():
                p_copy(1, lq).wait_recv()

            @pl.when(jnp.logical_not(last_of_part))
            def _():
                pout[1, lq] = pin[1, lq] + inc[1, lq]
                p_copy(1, lq).start()

        lr = t - begin2 - second_s

        @pl.when(inside(lr))
        def _():
            @pl.when(jnp.logical_not(source))
            def _():
                s_copy(1, lr).wait_recv()

            @pl.when(ring == 0)
            def _():
                @pl.when(z == last)
                def _():
                    sout[1, lr] = pin[1, lr] + inc[1, lr]
                    u_copy(lr).start()
                    s_copy(1, lr).start()
                    t_copy(1, lr).start()

                @pl.when(z < last)
                def _():
                    spread_copy(lr).start()

                @pl.when(jnp.logical_or(z < half - 2, jnp.logical_and(z >= half, z < last)))
                def _():
                    relay_copy(lr).start()

            @pl.when(ring == 1)
            def _():
                @pl.when(z == half - 1)
                def _():
                    sout[1, lr] = inc[1, lr]
                    s_copy(1, lr).start()

                @pl.when(z < half - 1)
                def _():
                    sout[1, lr] = sin[1, lr] + inc[1, lr]
                    s_copy(1, lr).start()

                @pl.when(z > half)
                def _():
                    relay_copy(lr).start()

        lf = t - begin2 - finish

        @pl.when(inside(lf))
        def _():
            @pl.when(ring == 1)
            def _():
                t_copy(1, lf).wait_recv()

            total = pin[1, lf] + tin[1, lf] + inc[1, lf]
            upper = jnp.logical_and(ring == 1, z >= half)

            @pl.when(upper)
            def _():
                out[row(lf), :] = anchor[row(lf), :] + (total + sin[1, lf])

            @pl.when(jnp.logical_not(upper))
            def _():
                out[row(lf), :] = anchor[row(lf), :] + total

        return carry

    lax.fori_loop(0, steps, step, 0)

    ends = jnp.logical_or(z == half - 1, z == half - 2)
    passes = jnp.where(ring == 0, jnp.logical_not(ends), z != half)

    def drain(l, carry):
        for s in range(2):
            halo_copy(s, 0, l).wait_send()
            halo_copy(s, 1, l).wait_send()

            @pl.when(ring == 0)
            def _():
                t_copy(s, l).wait_send()

        @pl.when(z < last)
        def _():
            p_copy(0, l).wait_send()

        @pl.when(jnp.logical_not(last_of_part))
        def _():
            p_copy(1, l).wait_send()

        @pl.when(jnp.logical_and(ring == 0, z > 0))
        def _():
            s_copy(0, l).wait_send()

        @pl.when(passes)
        def _():
            s_copy(1, l).wait_send()

        @pl.when(jnp.logical_and(ring == 0, z == last))
        def _():
            u_copy(l).wait_send()

        return carry

    lax.fori_loop(0, lats, drain, 0)


def rows_of(field):
    lats, cin, width = field.shape
    return field.transpose(1, 0, 2).reshape(cin * lats, width)


def body(window, anchor, noise, conv_in, conv_out, time_shift, plan, start):
    _, lats, cin, width = window.shape
    hidden = time_shift.shape[0]
    vmem = pl.BlockSpec(memory_space=pltpu.VMEM)
    smem = pl.BlockSpec(memory_space=pltpu.SMEM)
    hbm = pl.BlockSpec(memory_space=pl.ANY)
    rows = (2, lats, cin, width)
    dma = pltpu.SemaphoreType.DMA
    out = pl.pallas_call(
        kernel,
        out_shape=jax.ShapeDtypeStruct((cin * lats, width), F32),
        in_specs=[hbm] * 5 + [vmem] + [smem] * 2,
        out_specs=vmem,
        scratch_shapes=[pltpu.VMEM((cin * lats, width), F32)] * 3
        + [
            pltpu.VMEM((3, 3, cin, hidden), BF16),
            pltpu.VMEM((3, 3, cin, hidden), BF16),
            dma((5,)),
            pltpu.VMEM(rows, BF16),
            pltpu.VMEM((2,) + rows, BF16),
            pltpu.VMEM((2, lats + 2, 256, 2 * width), BF16),
            pltpu.VMEM((2, lats + 2, hidden, 2 * width), BF16),
            pltpu.VMEM((3, hidden, 256), BF16),
            pltpu.VMEM((3, 240, hidden), BF16),
            pltpu.VMEM((3, 256, hidden), BF16),
            pltpu.VMEM((3, 8, width), F32),
            pltpu.VMEM((hidden, width), F32),
            pltpu.VMEM((lats, cin, width), F32),
            pltpu.VMEM(rows, F32),
        ]
        + [pltpu.VMEM(rows, F32)] * 6
        + [dma((2, 2, lats))] * 2
        + [dma((2, lats))] * 6
        + [dma((lats,))],
        compiler_params=pltpu.CompilerParams(
            collective_id=0, has_side_effects=True, vmem_limit_bytes=56 * 1024 * 1024
        ),
    )(
        rows_of(window[0]), rows_of(anchor), rows_of(noise[0]), conv_in.transpose(0, 1, 3, 2),
        conv_out, time_shift[None, :], plan, start,
    )
    return out.reshape(cin, lats, width).transpose(1, 0, 2)[None]


def solution(mesh):
    return jax.shard_map(
        body,
        mesh=mesh,
        in_specs=(
            P("lvl", None, None, "lon"),
            P(None, None, "lon"),
            P("lvl", None, None, "lon"),
            P(),
            P(),
            P(),
            P(),
            P(),
        ),
        out_specs=P("lvl", None, None, "lon"),
        check_vma=False,
    )
```
